32 devices in a mesh: outer: 4 (over x, core), chip: 8 (over z, y).
Axes of the slice: x: 2, y: 2, z: 4, core: 2. Of those that a mesh axis runs over, the one named last changes fastest.
Arguments:
- inputs: bfloat16 [4096, 2048], P(('outer', 'chip')), may hold values from -6 to 6
- out_grads: bfloat16 [4096, 2048], P(('outer', 'chip')), may hold values from -6 to 6
- weight: bfloat16 [2048, 2048], P('chip'), may hold values from -0.125 to 0.125
- start_basis: float32 [64, 2048], P('chip'), may hold values from -6 to 6
- error_buffer: float32 [4, 2048, 2048], P('outer', 'chip'), may hold values from -2 to 2
Outputs:
- outputs: bfloat16 [4096, 2048], P(('outer', 'chip'))
- new_error: float32 [4, 2048, 2048], P('outer', 'chip')
The draws below stay inside these ranges and needn't reach their ends.
All inputs are finite; a program needn't handle non-finite values.
Results may differ from the reference program's by a relative error of at most 0.0085.
Values may be sent and summed in bfloat16 or wider, within the bound.
A program may use at most 128 MiB of HBM per device.

```python
import jax
import jax.numpy as jnp
from jax import lax

D = 2048
INNER = 2048
RANK = 8
TOK_DEV = 128
PODS = 4
QROWS = 64
TOKENS = 4096
N_CHIP = 8


def block_levels(own_key, extent, shards, least, high):
    def one(position, parts):
        draws = jax.random.uniform(jax.random.fold_in(jax.random.fold_in(own_key, 6), position), (parts,), jnp.float32, least / len(shards), high / len(shards))
        return jnp.repeat(jnp.exp(draws), extent[position] // parts).reshape((-1,) + (1,) * (len(extent) - position - 1))

    factor_of = one(*shards[0])
    for cut in shards[1:]:
        factor_of = factor_of * one(*cut)
    return factor_of


def centred(key, extent, scale, reach, shards=(), kind=jnp.bfloat16):
    level = block_levels(key, extent, shards, -0.22, 0.18) if shards else 1.0
    array = jax.random.normal(key, extent, jnp.float32) * scale * level
    return jnp.minimum(jnp.maximum(array, -reach), reach).astype(kind)


def setup_inputs(seed: int = 0) -> dict:
    keys = jax.random.split(jax.random.key(seed), 6)
    return {
        "inputs": centred(keys[0], (TOKENS, D), 1.0, 6.0, ((0, 32),)),
        "out_grads": centred(keys[1], (TOKENS, INNER), 1.0, 6.0, ((0, 32),)),
        "weight": centred(keys[2], (D, INNER), D ** -0.5, 0.125, ((0, 8),)),
        "start_basis": centred(keys[3], (QROWS, INNER), 1.0, 6.0, ((0, 8),), jnp.float32),
        "error_buffer": centred(keys[4], (PODS, D, INNER), 0.25, 2.0, ((0, 4), (1, 8)), jnp.float32),
    }


LEARNING_RATE = 0.2

def orthonormal(projected):
    finished = []
    for index in range(projected.shape[-2]):
        vector = projected[..., index, :]
        for unit in finished:
            vector = vector - lax.optimization_barrier(jnp.sum(vector * unit, axis=-1, keepdims=True)) * unit
        finished.append(vector / jnp.sqrt(lax.optimization_barrier(jnp.sum(vector * vector, axis=-1, keepdims=True)) + 1.0))
    return jnp.stack(finished, axis=-2)

def reference(inputs, out_grads, weight, start_basis, error_buffer):
    highest = lax.Precision.HIGHEST
    shard_rows = D // N_CHIP
    pod_tokens = TOK_DEV * N_CHIP
    basis_in = start_basis.reshape(N_CHIP, RANK, INNER)
    merged_all = []
    left_sum = jnp.zeros((N_CHIP, RANK, shard_rows), jnp.float32)
    for pod in range(PODS):
        pod_inputs = inputs[pod * pod_tokens:(pod + 1) * pod_tokens]
        pod_grads = out_grads[pod * pod_tokens:(pod + 1) * pod_tokens]
        gradient = lax.dot_general(pod_inputs, pod_grads, (((0,), (0,)), ((), ())), preferred_element_type=jnp.float32) / TOK_DEV
        merged = (gradient + error_buffer[pod]).reshape(N_CHIP, shard_rows, INNER)
        merged_all.append(merged)
        left_sum = left_sum + jnp.einsum('cki,cri->ckr', basis_in, merged, precision=highest)
    left_basis = orthonormal(left_sum / PODS)
    right_sum = jnp.zeros((N_CHIP, RANK, INNER), jnp.float32)
    for merged in merged_all:
        right_sum = right_sum + jnp.einsum('ckr,cri->cki', left_basis, merged, precision=highest)
    right_factor = right_sum / PODS
    approx = jnp.einsum('ckr,cki->cri', left_basis, right_factor, precision=highest)
    new_error = jnp.stack([merged - approx for merged in merged_all]).reshape(PODS, D, INNER)
    new_weight = (weight.astype(jnp.float32) - LEARNING_RATE * approx.reshape(D, INNER)).astype(jnp.bfloat16)
    outputs = jnp.dot(inputs, new_weight, preferred_element_type=jnp.float32).astype(jnp.bfloat16)
    return (outputs, new_error)
```

```python
import functools

import jax
import jax.numpy as jnp
from jax import lax
from jax.experimental import pallas as pl
from jax.experimental.pallas import tpu as pltpu
from jax.sharding import PartitionSpec as P

TOK_DEV = 128
LEARNING_RATE = 0.2
CHUNKS = 4
F32 = jnp.float32
BF16 = jnp.bfloat16
HIGHEST = lax.Precision.HIGHEST


def dot(a, b, ca, cb, precision=None):
    return lax.dot_general(
        a, b, (((ca,), (cb,)), ((), ())), precision=precision, preferred_element_type=F32
    )


def orthonormal(v):
    count = v.shape[0]
    row = lax.broadcasted_iota(jnp.int32, (count, 1), 0)
    for k in range(count):
        pivot = v[k : k + 1, :]
        d = jnp.sum(v * pivot, axis=1, keepdims=True)
        norm = d[k : k + 1, :] + 1.0
        scale = jnp.where(row > k, d / norm, 0.0)
        unit = pivot / jnp.sqrt(norm)
        v = jnp.where(row == k, unit, v - scale * pivot)
    return v


def kernel(
    A, B, PODS,
    x_ref, g_ref, w_ref, basis_ref, err_ref,
    out_ref, ne_ref,
    xg, xt, gg, wq, ysend, yrecv, up_s, up_r, dn_s, dn_r,
    left_s, left_r, right_s, right_r, fl, fr,
    xs_sem, xr_sem, ws_sem, wr_sem, gs_sem, gr_sem, ys_sem, yr_sem, rs_sem, rr_sem,
    ls_sem, lr_sem, hs_sem, hr_sem, fs_sem, fq_sem,
):
    o = lax.axis_index("outer")
    c = lax.axis_index("chip")
    a, b = c // B, c % B
    NC = A * B
    T, N = g_ref.shape
    S = w_ref.shape[0]
    Q = B * S
    R = basis_ref.shape[0]
    K = CHUNKS
    CN = N // K
    cols = [pl.ds(k * CN, CN) for k in range(K)]

    def remote(src, dst, ss, rs, axis, index):
        return pltpu.make_async_remote_copy(
            src_ref=src, dst_ref=dst, send_sem=ss, recv_sem=rs,
            device_id={axis: index}, device_id_type=pl.DeviceIdType.MESH,
        )

    barrier = pltpu.get_barrier_semaphore()
    for d in range(1, NC):
        pl.semaphore_signal(
            barrier, inc=1, device_id={"chip": (c + d) % NC}, device_id_type=pl.DeviceIdType.MESH
        )
    for d in range(1, PODS):
        pl.semaphore_signal(
            barrier, inc=1, device_id={"outer": (o + d) % PODS}, device_id_type=pl.DeviceIdType.MESH
        )
    pl.semaphore_wait(barrier, NC - 1 + PODS - 1)

    def rows_of(s):
        return pl.ds(pl.multiple_of(s * T, T), T)

    def shard_of(s):
        return pl.ds(pl.multiple_of(s * S, S), S)

    x_copies = []
    for d in range(1, A):
        t = (a + d) % A
        x_copies.append(remote(
            x_ref.at[:, pl.ds(pl.multiple_of(t * Q, Q), Q)], xg.at[rows_of(a)],
            xs_sem.at[d], xr_sem.at[d], "chip", t * B + b,
        ))
    for cp in x_copies:
        cp.start()

    def g_copy(direction, h, k):
        step = 1 if direction == 0 else -1
        source = a - step * (h - 1)
        src = g_ref.at[:, cols[k]] if h == 1 else gg.at[rows_of(source), cols[k]]
        return remote(
            src, gg.at[rows_of(source), cols[k]],
            gs_sem.at[direction, h, k], gr_sem.at[direction, h, k], "chip", c + step * B,
        )

    def g_sends(direction, h):
        return (
            jnp.logical_and(a - (h - 1) >= 0, a + 1 < A)
            if direction == 0
            else jnp.logical_and(a + (h - 1) < A, a >= 1)
        )

    def g_gets(direction, h):
        return a - h >= 0 if direction == 0 else a + h < A

    def g_arrival(direction, h, k):
        step = 1 if direction == 0 else -1
        place = gg.at[rows_of(a - step * h), cols[k]]
        return remote(
            place, place, gs_sem.at[direction, h, k], gr_sem.at[direction, h, k], "chip",
            c - step * B,
        )

    for k in range(K):
        for direction in range(2):
            @pl.when(g_sends(direction, 1))
            def _():
                g_copy(direction, 1, k).start()

    w_copies = []
    for d in range(1, B):
        t = (b + d) % B
        w_copies.append(remote(
            w_ref, wq.at[shard_of(b)], ws_sem.at[d], wr_sem.at[d], "chip", a * B + t
        ))
    for cp in w_copies:
        cp.start()

    xg[rows_of(a), :] = x_ref[:, pl.ds(pl.multiple_of(a * Q, Q), Q)]
    gg[rows_of(a), :] = g_ref[...]
    wq[shard_of(b), :] = w_ref[...]
    for cp in x_copies:
        cp.wait_recv()
    xt[...] = xg[...].T

    def y_copy(d, k):
        t = (b + d) % B
        return remote(
            ysend.at[d, :, cols[k]], yrecv.at[d, :, cols[k]],
            ys_sem.at[d, k], yr_sem.at[d, k], "chip", a * B + t,
        )

    def gradient_chunk(k):
        for d in range(1, B):
            t = (b + d) % B
            part = dot(xt[shard_of(t), :], gg[:, cols[k]], 1, 0)
            ysend[d, :, cols[k]] = part.astype(BF16)
            y_copy(d, k).start()
        part = dot(xt[shard_of(b), :], gg[:, cols[k]], 1, 0)
        ne_ref[:, cols[k]] = part

    for wave in range(1, A - 1 + K):
        for h in range(1, A):
            k = wave - h
            if 0 <= k < K:
                for direction in range(2):
                    @pl.when(g_gets(direction, h))
                    def _():
                        g_arrival(direction, h, k).wait_recv()
                    if h + 1 < A:
                        @pl.when(g_sends(direction, h + 1))
                        def _():
                            g_copy(direction, h + 1, k).start()
        if 0 <= wave - (A - 1) < K:
            gradient_chunk(wave - (A - 1))

    def o_copy(direction, r, k):
        s_buf, r_buf = (up_s, up_r) if direction == 0 else (dn_s, dn_r)
        return remote(
            s_buf.at[r, :, cols[k]], r_buf.at[r, :, cols[k]],
            rs_sem.at[direction, r, k], rr_sem.at[direction, r, k], "chip",
            c + B if direction == 0 else c - B,
        )

    def o_sends(direction, r):
        return a + r < A if direction == 0 else a - r >= 0

    def o_gets(direction, r):
        if direction == 0:
            return jnp.logical_and(a >= 1, a - 1 + r < A)
        return jnp.logical_and(a + 1 < A, a + 1 - r >= 0)

    def out_stage(r):
        for k in range(K):
            for direction in range(2):
                s_buf, r_buf = (up_s, up_r) if direction == 0 else (dn_s, dn_r)

                @pl.when(o_sends(direction, r))
                def _():
                    token = a + r if direction == 0 else a - r
                    s_buf[r, :, cols[k]] = dot(xg[rows_of(token), :], wq[:, cols[k]], 1, 0).astype(BF16)
                    if r + 1 < A:
                        @pl.when(o_gets(direction, r + 1))
                        def _():
                            o_copy(direction, r + 1, k).wait_recv()
                            s_buf[r, :, cols[k]] = (
                                s_buf[r, :, cols[k]].astype(F32) + r_buf[r + 1, :, cols[k]].astype(F32)
                            ).astype(BF16)
                    o_copy(direction, r, k).start()

    for cp in w_copies:
        cp.wait_recv()
    out_stage(A - 1)

    total = None
    for k in range(K):
        part = ne_ref[:, cols[k]]
        for d in range(1, B):
            y_copy(d, k).wait_recv()
            part = part + yrecv[d, :, cols[k]].astype(F32)
        part = part / TOK_DEV + err_ref[:, cols[k]]
        ne_ref[:, cols[k]] = part
        piece = dot(basis_ref[:, cols[k]], part, 1, 1, HIGHEST)
        total = piece if total is None else total + piece
    left_s[...] = total
    l_copies = [
        remote(left_s, left_r.at[d], ls_sem.at[d], lr_sem.at[d], "outer", (o + d) % PODS)
        for d in range(1, PODS)
    ]
    for cp in l_copies:
        cp.start()
    for r in range(A - 2, 1, -1):
        out_stage(r)
    for d, cp in enumerate(l_copies):
        cp.wait_recv()
        total = total + left_r[d + 1]
    left = orthonormal(total / PODS)

    f_peers = [(c + d) % NC for d in range(1, NC)]
    fl[0] = left
    fl_copies = [
        remote(fl.at[0], fl.at[d + 1], fs_sem.at[0, d], fq_sem.at[0, d], "chip", t)
        for d, t in enumerate(f_peers)
    ]
    right = dot(left, ne_ref[...], 1, 0, HIGHEST).astype(BF16)
    right_s[...] = right
    h_copies = [
        remote(right_s, right_r.at[d], hs_sem.at[d], hr_sem.at[d], "outer", (o + d) % PODS)
        for d in range(1, PODS)
    ]
    for cp in h_copies:
        cp.start()
    for cp in fl_copies:
        cp.start()
    if A > 1:
        out_stage(1)
    right = right.astype(F32)
    for d, cp in enumerate(h_copies):
        cp.wait_recv()
        right = right + right_r[d + 1].astype(F32)
    right = right / PODS
    fr[0] = right.astype(BF16)
    fr_copies = [
        remote(fr.at[0], fr.at[d + 1], fs_sem.at[1, d], fq_sem.at[1, d], "chip", t)
        for d, t in enumerate(f_peers)
    ]
    for cp in fr_copies:
        cp.start()
    for k in range(K):
        ne_ref[:, cols[k]] = ne_ref[:, cols[k]] - dot(
            left, right[:, k * CN : (k + 1) * CN], 0, 0, HIGHEST
        )

    z_rows = []
    for d in range(NC):
        if d > 0:
            fl_copies[d - 1].wait_recv()
        owner = (c - d + NC) % NC
        z_rows.append(dot(fl[d], x_ref[:, shard_of(owner)].astype(F32), 1, 1, HIGHEST))
    z = jnp.concatenate(z_rows, axis=0)
    for cp in fr_copies:
        cp.wait_recv()
    for k in range(K):
        rights = jnp.concatenate([fr[d, :, cols[k]].astype(F32) for d in range(NC)], axis=0)
        delta = dot(z, rights, 0, 0, HIGHEST)
        for direction in range(2):
            r_buf = up_r if direction == 0 else dn_r

            @pl.when(o_gets(direction, 1))
            def _():
                o_copy(direction, 1, k).wait_recv()

            @pl.when(jnp.logical_not(o_gets(direction, 1)))
            def _():
                r_buf[1, :, cols[k]] = jnp.zeros((T, CN), BF16)
        mine = dot(xg[rows_of(a), :], wq[:, cols[k]], 1, 0)
        mine = mine + up_r[1, :, cols[k]].astype(F32) + dn_r[1, :, cols[k]].astype(F32)
        out_ref[:, cols[k]] = (mine - LEARNING_RATE * delta).astype(BF16)

    for cp in x_copies + w_copies + l_copies + h_copies + fl_copies + fr_copies:
        cp.wait_send()
    for k in range(K):
        for d in range(1, B):
            y_copy(d, k).wait_send()
        for direction in range(2):
            for h in range(1, A):
                @pl.when(g_sends(direction, h))
                def _():
                    g_copy(direction, h, k).wait_send()

                @pl.when(o_sends(direction, h))
                def _():
                    o_copy(direction, h, k).wait_send()


def shards(inputs, out_grads, weight, start_basis, error_buffer):
    PODS, NC = lax.axis_size("outer"), lax.axis_size("chip")
    A = 4 if NC % 4 == 0 else NC
    B = NC // A
    T, D = inputs.shape
    N = out_grads.shape[1]
    S = weight.shape[0]
    R = start_basis.shape[0]
    Q = B * S
    K = CHUNKS
    dma = pltpu.SemaphoreType.DMA
    vmem = pl.BlockSpec(memory_space=pltpu.VMEM)
    outputs, new_error = pl.pallas_call(
        functools.partial(kernel, A, B, PODS),
        out_shape=(
            jax.ShapeDtypeStruct((T, N), BF16),
            jax.ShapeDtypeStruct((S, N), F32),
        ),
        in_specs=[vmem] * 5,
        out_specs=(vmem, vmem),
        scratch_shapes=[
            pltpu.VMEM((A * T, Q), BF16),
            pltpu.VMEM((Q, A * T), BF16),
            pltpu.VMEM((A * T, N), BF16),
            pltpu.VMEM((Q, N), BF16),
            pltpu.VMEM((B, S, N), BF16),
            pltpu.VMEM((B, S, N), BF16),
            pltpu.VMEM((A, T, N), BF16),
            pltpu.VMEM((A, T, N), BF16),
            pltpu.VMEM((A, T, N), BF16),
            pltpu.VMEM((A, T, N), BF16),
            pltpu.VMEM((R, S), F32),
            pltpu.VMEM((PODS, R, S), F32),
            pltpu.VMEM((R, N), BF16),
            pltpu.VMEM((PODS, R, N), BF16),
            pltpu.VMEM((NC, R, S), F32),
            pltpu.VMEM((NC, R, N), BF16),
            dma((A,)), dma((A,)), dma((B,)), dma((B,)),
            dma((2, A, K)), dma((2, A, K)), dma((B, K)), dma((B, K)),
            dma((2, A, K)), dma((2, A, K)),
            dma((PODS,)), dma((PODS,)), dma((PODS,)), dma((PODS,)),
            dma((2, NC)), dma((2, NC)),
        ],
        compiler_params=pltpu.CompilerParams(
            collective_id=0, has_side_effects=True, vmem_limit_bytes=56 * 1024 * 1024
        ),
        name="step",
    )(inputs, out_grads, weight, start_basis, error_buffer[0])
    return outputs, new_error[None]


def solution(mesh):
    return jax.shard_map(
        shards,
        mesh=mesh,
        in_specs=(
            P(("outer", "chip"), None),
            P(("outer", "chip"), None),
            P("chip", None),
            P("chip", None),
            P("outer", "chip", None),
        ),
        out_specs=(P(("outer", "chip"), None), P("outer", "chip", None)),
        check_vma=False,
    )
```
